32 devices in a mesh: src: 8 (over z, core), tgt: 4 (over y, x).
Axes of the slice: x: 2, y: 2, z: 4, core: 2. Of those that a mesh axis runs over, the one named last changes fastest.
Arguments:
- source_embed: bfloat16 [128, 128, 128], P('src', None, 'tgt'), may hold values from -4 to 4
- target_embed: bfloat16 [64, 128, 128], P('tgt', None, 'src'), may hold values from -4 to 4
- source_mass: float32 [128, 128], P('src'), may hold values from 10 to 14
- target_mass: float32 [64, 128], P('tgt'), may hold values from 10 to 14
- target_start: float32 [64, 128], P('tgt'), may hold values from -6 to 6
- block_pairs: int32 [8, 4, 128, 2], P('src', 'tgt'), may hold values from 0 to 15, as said below
- counts: int32 [8, 4], P('src', 'tgt'), may hold values from 16 to 128, as said below
Outputs:
- sender_log_scaling: float32 [128, 128], P('src')
- target_dual_potential: float32 [64, 128], P('tgt')
The draws below stay inside these ranges and needn't reach their ends.
Inputs may be any that keep to these rules, and one draw needn't show every extreme that they name: `block_pairs`: entry 0 of a slot is a local source block (below 16), entry 1 a local target block (below 16). The live slots of a device name distinct pairs; its first 16 slots name each of its target blocks once and each of its source blocks at least once. Slots at or past the device's count are not kept and hold arbitrary block numbers. `counts`: some device has all 128 slots live in every draw.
All inputs are finite; a program needn't handle non-finite values.
Results may differ from the reference program's by a relative error of at most 0.0003.
Values may be sent and summed in bfloat16 or wider, within the bound.
A program may use at most 64 MiB of HBM per device.

```python
import jax
import jax.numpy as jnp
from jax import lax

D = 128
BLK = 128
ITERS = 2
SB_DEV = 16
TB_DEV = 16
PAIRS = 128
SBLOCKS = 128
TBLOCKS = 64
N_SRC = 8
N_TGT = 4


def device_shifts(key):
    return jax.random.randint(jax.random.fold_in(key, 7), (N_SRC, N_TGT), 0, TB_DEV)


def draw_block_pairs(key, part):
    shifts = device_shifts(key).reshape(-1)
    grid_cell_index = lax.iota(jnp.int32, SB_DEV * TB_DEV)
    source_block = grid_cell_index // TB_DEV
    target_block = grid_cell_index % TB_DEV
    subkeys = jax.random.split(jax.random.fold_in(key, 8), N_SRC * N_TGT)

    def one_device(subkey, device_shift):
        offset = (target_block - device_shift) % TB_DEV
        leading = source_block == offset % SB_DEV
        ranking = jax.random.permutation(subkey, SB_DEV * TB_DEV).astype(jnp.int32)
        similarity_matrix = jnp.where(leading, ranking, SB_DEV * TB_DEV + ranking)
        ordering = jnp.argsort(similarity_matrix)[:PAIRS]
        return jnp.stack([source_block[ordering], target_block[ordering]], axis=1)
    enrolled_pairs = jax.vmap(one_device)(subkeys, shifts)
    return enrolled_pairs.reshape(N_SRC, N_TGT, PAIRS, 2).astype(jnp.int32)


def draw_counts(key, part):
    rolled = jax.random.randint(jax.random.fold_in(key, 9), (N_SRC * N_TGT,), 0, 17)
    loads = TB_DEV + (PAIRS - TB_DEV) * rolled * rolled * rolled // 4096
    hottest = jax.random.randint(jax.random.fold_in(key, 10), (), 0, N_SRC * N_TGT)
    loads = jnp.where(lax.iota(jnp.int32, N_SRC * N_TGT) == hottest, PAIRS, loads)
    return loads.reshape(N_SRC, N_TGT).astype(jnp.int32)


def embeddings(key):
    source_key = jax.random.fold_in(key, 21)
    target_key = jax.random.fold_in(key, 22)
    source_draw = jnp.clip(jax.random.normal(source_key, (SBLOCKS, BLK, D), jnp.float32), -4.0, 4.0)
    target_draw = jnp.clip(jax.random.normal(target_key, (TBLOCKS, BLK, D), jnp.float32), -4.0, 4.0)
    return (source_draw, target_draw)


def draw_source_embed(key, part):
    return embeddings(key)[0].astype(jnp.bfloat16)


def draw_target_embed(key, part):
    return embeddings(key)[1].astype(jnp.bfloat16)


def level_of(key, dims, shards, low, high):
    level, own = 1.0, jax.random.fold_in(key, 6)
    for dim, blocks in shards:
        steps = jnp.exp(jax.random.uniform(jax.random.fold_in(own, dim), (blocks,), jnp.float32, low / len(shards), high / len(shards)))
        level = level * jnp.repeat(steps, dims[dim] // blocks).reshape([-1 if axis == dim else 1 for axis in range(len(dims))])
    return level


def gaussian(stream_key, dims, deviation, most, pieces=(), held_as=jnp.bfloat16):
    result = deviation * jax.random.normal(stream_key, dims, jnp.float32)
    if pieces:
        result = result * level_of(stream_key, dims, pieces, -0.22, 0.18)
    return jnp.clip(result, -most, most).astype(held_as)


def setup_inputs(seed: int = 0) -> dict:
    seeds = jax.random.split(jax.random.key(seed), 8)
    source_embed = draw_source_embed(jax.random.fold_in(seeds[7], 71), 0)
    target_embed = draw_target_embed(jax.random.fold_in(seeds[7], 71), 0)
    source_mass = jnp.clip(10.0 + 4.0 * jax.random.uniform(seeds[2], (SBLOCKS, BLK), jnp.float32) ** level_of(seeds[2], (SBLOCKS, BLK), ((0, 8),), -0.2, 0.2), 10.0, 14.0)
    target_mass = jnp.clip(10.0 + 4.0 * jax.random.uniform(seeds[3], (TBLOCKS, BLK), jnp.float32) ** level_of(seeds[3], (TBLOCKS, BLK), ((0, 4),), -0.2, 0.2), 10.0, 14.0)
    target_start = gaussian(seeds[4], (TBLOCKS, BLK), 1.0, 6.0, ((0, 4),), jnp.float32)
    block_pairs = draw_block_pairs(jax.random.fold_in(seeds[7], 71), 0)
    counts = draw_counts(jax.random.fold_in(seeds[7], 71), 0)
    return dict(source_embed=source_embed, target_embed=target_embed, source_mass=source_mass, target_mass=target_mass, target_start=target_start, block_pairs=block_pairs, counts=counts)


smoothing_epsilon = 4.0
empty_peak = -1e30
list_batch = 64


def kept_list(block_pairs, counts):
    layout = block_pairs.shape[:3]
    device_src = lax.broadcasted_iota(jnp.int32, layout, 0)
    device_tgt = lax.broadcasted_iota(jnp.int32, layout, 1)
    slot_ids = lax.broadcasted_iota(jnp.int32, layout, 2)
    live = (slot_ids < counts[:, :, None]).reshape(-1)
    source_ids = (device_src * SB_DEV + block_pairs[..., 0]).reshape(-1).astype(jnp.int32)
    target_ids = (device_tgt * TB_DEV + block_pairs[..., 1]).reshape(-1).astype(jnp.int32)
    ordering = jnp.argsort(jnp.where(live, 0, 1).astype(jnp.int32), stable=True)
    total = jnp.sum(live.astype(jnp.int32)).astype(jnp.int32)
    padding = jnp.zeros((list_batch,), jnp.int32)
    source_ids = jnp.concatenate([source_ids[ordering], padding])
    target_ids = jnp.concatenate([target_ids[ordering], padding])
    live = jnp.concatenate([live[ordering], jnp.zeros((list_batch,), bool)])
    return source_ids, target_ids, live, total


def absorb(maxima, totals, targets, block_peak, block_total):
    raised = maxima.at[targets].max(block_peak)
    totals = totals * jnp.exp(maxima - raised)
    totals = totals.at[targets].add(block_total * jnp.exp(block_peak - raised[targets]))
    return raised, totals


def half_step(local_side, far_side, potential, local_ids, far_ids, live, total, log_mass):
    def group(counter, running):
        maxima, totals = running
        offset = (counter * list_batch).astype(jnp.int32)
        near = lax.dynamic_slice_in_dim(local_ids, offset, list_batch)
        distant = lax.dynamic_slice_in_dim(far_ids, offset, list_batch)
        usable = lax.dynamic_slice_in_dim(live, offset, list_batch)
        query_frame_vectors = local_side[near].astype(jnp.float32)
        reply_frame_vectors = far_side[distant].astype(jnp.float32)
        similarity_matrix = jnp.einsum("fdg,fwg->fdw", query_frame_vectors, reply_frame_vectors, precision=lax.Precision.HIGHEST) / smoothing_epsilon
        similarity_matrix = similarity_matrix + potential[distant][:, None, :]
        block_peak = jnp.max(similarity_matrix, axis=2)
        block_total = jnp.sum(jnp.exp(similarity_matrix - block_peak[:, :, None]), axis=2)
        block_peak = jnp.where(usable[:, None], block_peak, empty_peak)
        block_total = jnp.where(usable[:, None], block_total, 0.0)
        return absorb(maxima, totals, near, block_peak, block_total)

    groups = ((total + list_batch - 1) // list_batch).astype(jnp.int32)
    start_max = jnp.full(log_mass.shape, empty_peak, jnp.float32)
    start_sum = jnp.zeros(log_mass.shape, jnp.float32)
    maxima, totals = lax.fori_loop(jnp.int32(0), groups, group, (start_max, start_sum))
    return log_mass - (maxima + jnp.log(totals))


def reference(source_embed, target_embed, source_mass, target_mass, target_start, block_pairs, counts):
    source_ids, target_ids, live, total = kept_list(block_pairs, counts)
    target_dual_potential = target_start
    sender_log_scaling = source_mass
    for iteration in range(ITERS):
        sender_log_scaling = half_step(source_embed, target_embed, target_dual_potential, source_ids, target_ids, live, total, source_mass)
        target_dual_potential = half_step(target_embed, source_embed, sender_log_scaling, target_ids, source_ids, live, total, target_mass)
    return sender_log_scaling, target_dual_potential
```

```python
import functools
import math

import jax
import jax.numpy as jnp
from jax import lax
from jax.experimental import pallas as pl
from jax.experimental.pallas import tpu as pltpu
from jax.sharding import PartitionSpec as P

ITERS = 2

smoothing_epsilon = 4.0
dead_score = -1e30
log2_e = math.log2(math.e)
ln_2 = math.log(2.0)
column_group = 4
feature_tile = 16


def merge(parts):
    peak = functools.reduce(jnp.maximum, parts)
    total = functools.reduce(jnp.add, [jnp.exp2(part - peak) for part in parts])
    return peak + jnp.log2(total)


def kernel(
    n_src,
    n_tgt,
    gather_here,
    source_ref,
    target_ref,
    source_mass_ref,
    target_mass_ref,
    start_ref,
    plan_ref,
    count_ref,
    source_out,
    target_out,
    score,
    source_full,
    target_full,
    spread,
    bias,
    potential,
    row_parts,
    col_parts,
    own_sems,
    gs_send,
    gs_recv,
    gt_send,
    gt_recv,
    row_send,
    row_recv,
    col_send,
    col_recv,
):
    s, t = lax.axis_index("src"), lax.axis_index("tgt")
    source_blocks, target_blocks, frames, _ = score.shape
    sizes = {"src": n_src, "tgt": n_tgt}
    here = {"src": s, "tgt": t}

    def peer(axis, step):
        return lax.rem(here[axis] + step, sizes[axis])

    barrier = pltpu.get_barrier_semaphore()
    for axis in ("src", "tgt"):
        for step in range(1, sizes[axis]):
            pl.semaphore_signal(
                barrier,
                inc=1,
                device_id={axis: peer(axis, step)},
                device_id_type=pl.DeviceIdType.MESH,
            )
    pl.semaphore_wait(barrier, n_src + n_tgt - 2)

    def remote(src, dst, send, recv, axis, step):
        return pltpu.make_async_remote_copy(
            src_ref=src,
            dst_ref=dst,
            send_sem=send,
            recv_sem=recv,
            device_id={axis: peer(axis, step)},
            device_id_type=pl.DeviceIdType.MESH,
        )

    def gather_copies(local, full, send, recv, axis):
        width = local.shape[1]

        def slot(owner):
            return full.at[:, pl.ds(pl.multiple_of(owner * width, width), width), :]

        out, arrive = [], []
        for step in range(1, sizes[axis]):
            out.append(
                remote(local, slot(here[axis]), send.at[step], recv.at[step], axis, step)
            )
            sender = lax.rem(here[axis] + sizes[axis] - step, sizes[axis])
            arrive.append(
                remote(local, slot(sender), send.at[step], recv.at[step], axis, step)
            )
        return out, arrive, slot(here[axis])

    if gather_here:
        s_out, s_in, s_own = gather_copies(source_ref, source_full, gs_send, gs_recv, "tgt")
        t_out, t_in, t_own = gather_copies(target_ref, target_full, gt_send, gt_recv, "src")
        for copy in t_out + s_out:
            copy.start()
        own = [
            pltpu.make_async_copy(source_ref, s_own, own_sems.at[0]),
            pltpu.make_async_copy(target_ref, t_own, own_sems.at[1]),
        ]
    else:
        own = [
            pltpu.make_async_copy(source_ref, source_full, own_sems.at[0]),
            pltpu.make_async_copy(target_ref, target_full, own_sems.at[1]),
        ]
    for copy in own:
        copy.start()

    slots = plan_ref.shape[1]
    live = lax.broadcasted_iota(jnp.int32, (source_blocks, slots), 1) < count_ref[0, 0]
    near = lax.broadcasted_iota(jnp.int32, (source_blocks, slots), 0) == plan_ref[0:1, :]
    far = lax.broadcasted_iota(jnp.int32, (target_blocks, slots), 0) == plan_ref[1:2, :]
    near = jnp.where(near & live, 1.0, 0.0).astype(jnp.bfloat16)
    far = jnp.where(far, 1.0, 0.0).astype(jnp.bfloat16)
    kept = lax.dot_general(
        near, far, (((1,), (1,)), ((), ())), preferred_element_type=jnp.float32
    )
    for block in range(target_blocks):
        bias[block] = jnp.broadcast_to(
            jnp.where(kept[:, block : block + 1] > 0.5, 0.0, dead_score),
            (source_blocks, frames),
        )
    potential[...] = start_ref[...] * log2_e

    diagonal = lax.broadcasted_iota(jnp.int32, (frames, frames), 0) == (
        lax.broadcasted_iota(jnp.int32, (frames, frames), 1)
    )

    for copy in own:
        copy.wait()
    if gather_here:
        for copy in s_in + t_in:
            copy.wait_recv()

    def row_block(block, parts, make_scores):
        if make_scores:
            left = source_full[block].T
        peak = None
        for other in range(0, target_blocks, 2):
            if make_scores:
                right = jnp.concatenate(
                    [target_full[other], target_full[other + 1]], axis=1
                )
                product = jnp.dot(left, right, preferred_element_type=jnp.float32)
            for k in range(2):
                if make_scores:
                    tile = product[:, k * frames : (k + 1) * frames] * (
                        log2_e / smoothing_epsilon
                    ) + bias[other + k, pl.ds(block, 1), :]
                    score[block, other + k] = tile
                else:
                    tile = score[block, other + k]
                tile = tile + potential[other + k : other + k + 1, :]
                peak = tile if peak is None else jnp.maximum(peak, tile)
        peak = jnp.max(peak, axis=1, keepdims=True)
        total = None
        for other in range(target_blocks):
            term = jnp.exp2(
                score[block, other] + potential[other : other + 1, :] - peak
            )
            total = term if total is None else total + term
        total = jnp.sum(total, axis=1, keepdims=True)
        column = peak + jnp.log2(total)
        row = jnp.sum(jnp.where(diagonal, column, 0.0), axis=0, keepdims=True)
        parts[0, pl.ds(block, 1), :] = row

    def column_group_stats(first, parts):
        start = jnp.full((8, frames), 2 * dead_score, jnp.float32)

        def fold(value):
            return value.reshape(frames // 8, 8, frames)

        def tile(block, k):
            return score[block, first + k] + spread[block]

        def peaks(block, current):
            return tuple(
                jnp.maximum(current[k], jnp.max(fold(tile(block, k)), axis=0))
                for k in range(column_group)
            )

        peak = lax.fori_loop(0, source_blocks, peaks, (start,) * column_group)
        peak = [jnp.max(p, axis=0, keepdims=True) for p in peak]

        def sums(block, current):
            return tuple(
                current[k] + jnp.sum(fold(jnp.exp2(tile(block, k) - peak[k])), axis=0)
                for k in range(column_group)
            )

        total = lax.fori_loop(
            0, source_blocks, sums, (jnp.zeros((8, frames), jnp.float32),) * column_group
        )
        for k in range(column_group):
            parts[0, pl.ds(first + k, 1), :] = peak[k] + jnp.log2(
                jnp.sum(total[k], axis=0, keepdims=True)
            )

    sends = []

    def exchange(parts, send, recv, axis):
        copies = [
            remote(parts.at[0], parts.at[step], send.at[step], recv.at[step], axis, step)
            for step in range(1, sizes[axis])
        ]
        for copy in copies:
            copy.start()
        for copy in copies:
            copy.wait_recv()
        sends.extend(copies)
        return merge([parts[step] for step in range(sizes[axis])])

    for iteration in range(ITERS):
        parts = row_parts.at[iteration]

        def rows(block, carry):
            row_block(block, parts, iteration == 0)
            return carry

        lax.fori_loop(0, source_blocks, rows, 0)
        sender = source_mass_ref[...] * log2_e - exchange(
            parts, row_send.at[iteration], row_recv.at[iteration], "tgt"
        )
        if iteration == ITERS - 1:
            source_out[...] = sender * ln_2
        for block in range(source_blocks):
            column = jnp.sum(
                jnp.where(diagonal, sender[block : block + 1, :], 0.0),
                axis=1,
                keepdims=True,
            )
            spread[block] = jnp.broadcast_to(column, (frames, frames))
        parts = col_parts.at[iteration]

        def columns(group, carry):
            column_group_stats(group * column_group, parts)
            return carry

        lax.fori_loop(0, target_blocks // column_group, columns, 0)
        dual = target_mass_ref[...] * log2_e - exchange(
            parts, col_send.at[iteration], col_recv.at[iteration], "src"
        )
        if iteration == ITERS - 1:
            target_out[...] = dual * ln_2
        else:
            potential[...] = dual

    if gather_here:
        sends.extend(s_out + t_out)
    for copy in sends:
        copy.wait_send()


def on_device(
    n_src,
    n_tgt,
    source_embed,
    target_embed,
    source_mass,
    target_mass,
    target_start,
    block_pairs,
    counts,
):
    source = jnp.swapaxes(source_embed, 1, 2)
    target = jnp.swapaxes(target_embed, 1, 2)
    source_blocks, source_width, frames = source.shape
    target_blocks, target_width, _ = target.shape
    gather_here = source_width % feature_tile == 0 and target_width % feature_tile == 0
    if not gather_here:
        source = lax.all_gather(source, "tgt", axis=1, tiled=True)
        target = lax.all_gather(target, "src", axis=1, tiled=True)
    features = source_width * n_tgt
    plan = block_pairs.reshape(block_pairs.shape[2], 2).T
    dma = pltpu.SemaphoreType.DMA
    vmem = pl.BlockSpec(memory_space=pltpu.VMEM)
    return pl.pallas_call(
        functools.partial(kernel, n_src, n_tgt, gather_here),
        out_shape=(
            jax.ShapeDtypeStruct(source_mass.shape, jnp.float32),
            jax.ShapeDtypeStruct(target_mass.shape, jnp.float32),
        ),
        in_specs=[vmem] * 6 + [pl.BlockSpec(memory_space=pltpu.SMEM)],
        out_specs=(vmem, vmem),
        scratch_shapes=[
            pltpu.VMEM((source_blocks, target_blocks, frames, frames), jnp.float32),
            pltpu.VMEM((source_blocks, features, frames), jnp.bfloat16),
            pltpu.VMEM((target_blocks, features, frames), jnp.bfloat16),
            pltpu.VMEM((source_blocks, frames, frames), jnp.float32),
            pltpu.VMEM((target_blocks, source_blocks, frames), jnp.float32),
            pltpu.VMEM((target_blocks, frames), jnp.float32),
            pltpu.VMEM((ITERS, n_tgt, source_blocks, frames), jnp.float32),
            pltpu.VMEM((ITERS, n_src, target_blocks, frames), jnp.float32),
            dma((2,)),
            dma((n_tgt,)),
            dma((n_tgt,)),
            dma((n_src,)),
            dma((n_src,)),
            dma((ITERS, n_tgt)),
            dma((ITERS, n_tgt)),
            dma((ITERS, n_src)),
            dma((ITERS, n_src)),
        ],
        compiler_params=pltpu.CompilerParams(
            collective_id=0, has_side_effects=True, vmem_limit_bytes=40 * 2**20
        ),
        name="sinkhorn",
    )(source, target, source_mass, target_mass, target_start, plan, counts)


def solution(mesh):
    in_specs = (
        P("src", None, "tgt"),
        P("tgt", None, "src"),
        P("src", None),
        P("tgt", None),
        P("tgt", None),
        P("src", "tgt", None, None),
        P("src", "tgt"),
    )
    out_specs = (P("src", None), P("tgt", None))
    return jax.shard_map(
        functools.partial(on_device, mesh.shape["src"], mesh.shape["tgt"]),
        mesh=mesh,
        in_specs=in_specs,
        out_specs=out_specs,
        check_vma=False,
    )
```

```python
import functools
import math

import jax
import jax.numpy as jnp
from jax import lax
from jax.experimental import pallas as pl
from jax.experimental.pallas import tpu as pltpu
from jax.sharding import PartitionSpec as P

ITERS = 2

smoothing_epsilon = 4.0
dead_score = -1e30
log2_e = math.log2(math.e)
ln_2 = math.log(2.0)
column_group = 4
feature_tile = 16


def merge(parts):
    peak = functools.reduce(jnp.maximum, parts)
    total = functools.reduce(jnp.add, [jnp.exp2(part - peak) for part in parts])
    return peak + jnp.log2(total)


def kernel(
    n_src,
    n_tgt,
    gather_here,
    source_ref,
    target_ref,
    source_mass_ref,
    target_mass_ref,
    start_ref,
    plan_ref,
    count_ref,
    source_out,
    target_out,
    score,
    source_full,
    target_full,
    spread,
    bias,
    potential,
    row_parts,
    col_parts,
    own_sems,
    gs_send,
    gs_recv,
    gt_send,
    gt_recv,
    row_send,
    row_recv,
    col_send,
    col_recv,
):
    s, t = lax.axis_index("src"), lax.axis_index("tgt")
    source_blocks, target_blocks, frames, _ = score.shape
    sizes = {"src": n_src, "tgt": n_tgt}
    here = {"src": s, "tgt": t}

    def peer(axis, step):
        return lax.rem(here[axis] + step, sizes[axis])

    barrier = pltpu.get_barrier_semaphore()
    for axis in ("src", "tgt"):
        for step in range(1, sizes[axis]):
            pl.semaphore_signal(
                barrier,
                inc=1,
                device_id={axis: peer(axis, step)},
                device_id_type=pl.DeviceIdType.MESH,
            )
    pl.semaphore_wait(barrier, n_src + n_tgt - 2)

    def remote(src, dst, send, recv, axis, step):
        return pltpu.make_async_remote_copy(
            src_ref=src,
            dst_ref=dst,
            send_sem=send,
            recv_sem=recv,
            device_id={axis: peer(axis, step)},
            device_id_type=pl.DeviceIdType.MESH,
        )

    def gather_copies(local, full, send, recv, axis):
        width = local.shape[1]

        def slot(owner):
            return full.at[:, pl.ds(pl.multiple_of(owner * width, width), width), :]

        out, arrive = [], []
        for step in range(1, sizes[axis]):
            out.append(
                remote(local, slot(here[axis]), send.at[step], recv.at[step], axis, step)
            )
            sender = lax.rem(here[axis] + sizes[axis] - step, sizes[axis])
            arrive.append(
                remote(local, slot(sender), send.at[step], recv.at[step], axis, step)
            )
        return out, arrive, slot(here[axis])

    if gather_here:
        s_out, s_in, s_own = gather_copies(source_ref, source_full, gs_send, gs_recv, "tgt")
        width = target_ref.shape[1]
        partner = s + 1 - 2 * lax.rem(s, 2)

        def target_slot(owner):
            return target_full.at[:, pl.ds(pl.multiple_of(owner * width, width), width), :]

        def target_copy(src, owner, index, device):
            return pltpu.make_async_remote_copy(
                src_ref=src,
                dst_ref=target_slot(owner),
                send_sem=gt_send.at[index],
                recv_sem=gt_recv.at[index],
                device_id={"src": device},
                device_id_type=pl.DeviceIdType.MESH,
            )

        t_own = target_slot(s)
        t_out = [
            target_copy(target_ref, s, step, peer("src", step))
            for step in range(2, n_src, 2)
        ]
        for copy in t_out + s_out:
            copy.start()
        across = target_copy(target_ref, s, 1, partner)
        across.start()
        t_out.append(across)
        t_in = [target_copy(target_ref, partner, 1, partner)]
        own = [
            pltpu.make_async_copy(source_ref, s_own, own_sems.at[0]),
            pltpu.make_async_copy(target_ref, t_own, own_sems.at[1]),
        ]
    else:
        own = [
            pltpu.make_async_copy(source_ref, source_full, own_sems.at[0]),
            pltpu.make_async_copy(target_ref, target_full, own_sems.at[1]),
        ]
    for copy in own:
        copy.start()

    slots = plan_ref.shape[1]
    live = lax.broadcasted_iota(jnp.int32, (source_blocks, slots), 1) < count_ref[0, 0]
    near = lax.broadcasted_iota(jnp.int32, (source_blocks, slots), 0) == plan_ref[0:1, :]
    far = lax.broadcasted_iota(jnp.int32, (target_blocks, slots), 0) == plan_ref[1:2, :]
    near = jnp.where(near & live, 1.0, 0.0).astype(jnp.bfloat16)
    far = jnp.where(far, 1.0, 0.0).astype(jnp.bfloat16)
    kept = lax.dot_general(
        near, far, (((1,), (1,)), ((), ())), preferred_element_type=jnp.float32
    )
    for block in range(target_blocks):
        bias[block] = jnp.broadcast_to(
            jnp.where(kept[:, block : block + 1] > 0.5, 0.0, dead_score),
            (source_blocks, frames),
        )
    dual = start_ref[...] * log2_e
    sender = None
    potential[...] = dual

    diagonal = lax.broadcasted_iota(jnp.int32, (frames, frames), 0) == (
        lax.broadcasted_iota(jnp.int32, (frames, frames), 1)
    )

    for copy in own:
        copy.wait()
    if gather_here:
        for step in range(2, n_src, 2):
            owner = lax.rem(s + n_src - step, n_src)
            target_copy(target_ref, owner, step, owner).wait_recv()
            relay = target_copy(target_slot(owner), owner, step + 1, partner)
            relay.start()
            t_out.append(relay)
            owner = lax.rem(partner + n_src - step, n_src)
            t_in.append(target_copy(target_ref, owner, step + 1, partner))
        for copy in s_in + t_in:
            copy.wait_recv()

    def row_block(block, parts, make_scores):
        if make_scores:
            left = source_full[block].T
        peak = None
        for other in range(0, target_blocks, 2):
            if make_scores:
                right = jnp.concatenate(
                    [target_full[other], target_full[other + 1]], axis=1
                )
                product = jnp.dot(left, right, preferred_element_type=jnp.float32)
            for k in range(2):
                if make_scores:
                    tile = product[:, k * frames : (k + 1) * frames] * (
                        log2_e / smoothing_epsilon
                    ) + bias[other + k, pl.ds(block, 1), :]
                else:
                    tile = score[block, other + k]
                tile = tile + potential[other + k : other + k + 1, :]
                score[block, other + k] = tile
                peak = tile if peak is None else jnp.maximum(peak, tile)
        peak = jnp.max(peak, axis=1, keepdims=True)
        total = None
        for other in range(target_blocks):
            term = jnp.exp2(score[block, other] - peak)
            total = term if total is None else total + term
        total = jnp.sum(total, axis=1, keepdims=True)
        column = peak + jnp.log2(total)
        row = jnp.sum(jnp.where(diagonal, column, 0.0), axis=0, keepdims=True)
        parts[0, pl.ds(block, 1), :] = row

    def column_group_stats(first, parts):
        start = jnp.full((8, frames), 2 * dead_score, jnp.float32)

        def fold(value):
            return value.reshape(frames // 8, 8, frames)

        def peaks(block, current):
            raised = []
            for k in range(column_group):
                tile = score[block, first + k] + spread[block]
                score[block, first + k] = tile
                raised.append(jnp.maximum(current[k], jnp.max(fold(tile), axis=0)))
            return tuple(raised)

        peak = lax.fori_loop(0, source_blocks, peaks, (start,) * column_group)
        peak = [jnp.max(p, axis=0, keepdims=True) for p in peak]

        def sums(block, current):
            return tuple(
                current[k]
                + jnp.sum(fold(jnp.exp2(score[block, first + k] - peak[k])), axis=0)
                for k in range(column_group)
            )

        total = lax.fori_loop(
            0, source_blocks, sums, (jnp.zeros((8, frames), jnp.float32),) * column_group
        )
        for k in range(column_group):
            parts[0, pl.ds(first + k, 1), :] = peak[k] + jnp.log2(
                jnp.sum(total[k], axis=0, keepdims=True)
            )

    sends = []

    def exchange(parts, send, recv, axis):
        copies = [
            remote(parts.at[0], parts.at[step], send.at[step], recv.at[step], axis, step)
            for step in range(1, sizes[axis])
        ]
        for copy in copies:
            copy.start()
        for copy in copies:
            copy.wait_recv()
        sends.extend(copies)
        return merge([parts[step] for step in range(sizes[axis])])

    for iteration in range(ITERS):
        parts = row_parts.at[iteration]

        def rows(block, carry):
            row_block(block, parts, iteration == 0)
            return carry

        lax.fori_loop(0, source_blocks, rows, 0)
        fresh = source_mass_ref[...] * log2_e - exchange(
            parts, row_send.at[iteration], row_recv.at[iteration], "tgt"
        )
        if sender is None:
            shift = sender = fresh
        else:
            shift, sender = fresh, fresh + sender
        if iteration == ITERS - 1:
            source_out[...] = sender * ln_2
        for block in range(source_blocks):
            column = jnp.sum(
                jnp.where(diagonal, shift[block : block + 1, :], 0.0),
                axis=1,
                keepdims=True,
            )
            spread[block] = jnp.broadcast_to(column, (frames, frames))
        parts = col_parts.at[iteration]

        def columns(group, carry):
            column_group_stats(group * column_group, parts)
            return carry

        lax.fori_loop(0, target_blocks // column_group, columns, 0)
        fresh = target_mass_ref[...] * log2_e - exchange(
            parts, col_send.at[iteration], col_recv.at[iteration], "src"
        )
        dual = fresh + dual
        if iteration == ITERS - 1:
            target_out[...] = dual * ln_2
        else:
            potential[...] = fresh

    if gather_here:
        sends.extend(s_out + t_out)
    for copy in sends:
        copy.wait_send()


def on_device(
    n_src,
    n_tgt,
    source_embed,
    target_embed,
    source_mass,
    target_mass,
    target_start,
    block_pairs,
    counts,
):
    source = jnp.swapaxes(source_embed, 1, 2)
    target = jnp.swapaxes(target_embed, 1, 2)
    source_blocks, source_width, frames = source.shape
    target_blocks, target_width, _ = target.shape
    gather_here = source_width % feature_tile == 0 and target_width % feature_tile == 0
    if not gather_here:
        source = lax.all_gather(source, "tgt", axis=1, tiled=True)
        target = lax.all_gather(target, "src", axis=1, tiled=True)
    features = source_width * n_tgt
    plan = block_pairs.reshape(block_pairs.shape[2], 2).T
    dma = pltpu.SemaphoreType.DMA
    vmem = pl.BlockSpec(memory_space=pltpu.VMEM)
    return pl.pallas_call(
        functools.partial(kernel, n_src, n_tgt, gather_here),
        out_shape=(
            jax.ShapeDtypeStruct(source_mass.shape, jnp.float32),
            jax.ShapeDtypeStruct(target_mass.shape, jnp.float32),
        ),
        in_specs=[vmem] * 6 + [pl.BlockSpec(memory_space=pltpu.SMEM)],
        out_specs=(vmem, vmem),
        scratch_shapes=[
            pltpu.VMEM((source_blocks, target_blocks, frames, frames), jnp.float32),
            pltpu.VMEM((source_blocks, features, frames), jnp.bfloat16),
            pltpu.VMEM((target_blocks, features, frames), jnp.bfloat16),
            pltpu.VMEM((source_blocks, frames, frames), jnp.float32),
            pltpu.VMEM((target_blocks, source_blocks, frames), jnp.float32),
            pltpu.VMEM((target_blocks, frames), jnp.float32),
            pltpu.VMEM((ITERS, n_tgt, source_blocks, frames), jnp.float32),
            pltpu.VMEM((ITERS, n_src, target_blocks, frames), jnp.float32),
            dma((2,)),
            dma((n_tgt,)),
            dma((n_tgt,)),
            dma((n_src,)),
            dma((n_src,)),
            dma((ITERS, n_tgt)),
            dma((ITERS, n_tgt)),
            dma((ITERS, n_src)),
            dma((ITERS, n_src)),
        ],
        compiler_params=pltpu.CompilerParams(
            collective_id=0, has_side_effects=True, vmem_limit_bytes=40 * 2**20
        ),
        name="sinkhorn",
    )(source, target, source_mass, target_mass, target_start, plan, counts)


def solution(mesh):
    in_specs = (
        P("src", None, "tgt"),
        P("tgt", None, "src"),
        P("src", None),
        P("tgt", None),
        P("tgt", None),
        P("src", "tgt", None, None),
        P("src", "tgt"),
    )
    out_specs = (P("src", None), P("tgt", None))
    return jax.shard_map(
        functools.partial(on_device, mesh.shape["src"], mesh.shape["tgt"]),
        mesh=mesh,
        in_specs=in_specs,
        out_specs=out_specs,
        check_vma=False,
    )
```

```python
import functools
import math

import jax
import jax.numpy as jnp
from jax import lax
from jax.experimental import pallas as pl
from jax.experimental.pallas import tpu as pltpu
from jax.sharding import PartitionSpec as P

ITERS = 2

smoothing_epsilon = 4.0
dead_score = -1e30
log2_e = math.log2(math.e)
ln_2 = math.log(2.0)
column_group = 4
feature_tile = 16


def merge(parts):
    peak = functools.reduce(jnp.maximum, parts)
    total = functools.reduce(jnp.add, [jnp.exp2(part - peak) for part in parts])
    return peak + jnp.log2(total)


def kernel(
    n_src,
    n_tgt,
    gather_here,
    source_ref,
    target_ref,
    source_mass_ref,
    target_mass_ref,
    start_ref,
    plan_ref,
    count_ref,
    source_out,
    target_out,
    score,
    source_full,
    target_full,
    spread,
    bias,
    potential,
    row_parts,
    col_parts,
    own_sems,
    gs_send,
    gs_recv,
    gt_send,
    gt_recv,
    row_send,
    row_recv,
    col_send,
    col_recv,
):
    s, t = lax.axis_index("src"), lax.axis_index("tgt")
    source_blocks, target_blocks, frames, _ = score.shape
    sizes = {"src": n_src, "tgt": n_tgt}
    here = {"src": s, "tgt": t}

    def peer(axis, step):
        return lax.rem(here[axis] + step, sizes[axis])

    barrier = pltpu.get_barrier_semaphore()
    for axis in ("src", "tgt"):
        for step in range(1, sizes[axis]):
            pl.semaphore_signal(
                barrier,
                inc=1,
                device_id={axis: peer(axis, step)},
                device_id_type=pl.DeviceIdType.MESH,
            )
    pl.semaphore_wait(barrier, n_src + n_tgt - 2)

    def remote(src, dst, send, recv, axis, step):
        return pltpu.make_async_remote_copy(
            src_ref=src,
            dst_ref=dst,
            send_sem=send,
            recv_sem=recv,
            device_id={axis: peer(axis, step)},
            device_id_type=pl.DeviceIdType.MESH,
        )

    def gather_copies(local, full, send, recv, axis):
        width = local.shape[1]

        def slot(owner):
            return full.at[:, pl.ds(pl.multiple_of(owner * width, width), width), :]

        out, arrive = [], []
        for step in range(1, sizes[axis]):
            out.append(
                remote(local, slot(here[axis]), send.at[step], recv.at[step], axis, step)
            )
            sender = lax.rem(here[axis] + sizes[axis] - step, sizes[axis])
            arrive.append(
                remote(local, slot(sender), send.at[step], recv.at[step], axis, step)
            )
        return out, arrive, slot(here[axis])

    if gather_here:
        s_out, s_in, s_own = gather_copies(source_ref, source_full, gs_send, gs_recv, "tgt")
        width = target_ref.shape[1]
        partner = s + 1 - 2 * lax.rem(s, 2)

        def target_slot(owner):
            return target_full.at[:, pl.ds(pl.multiple_of(owner * width, width), width), :]

        def target_copy(src, owner, index, device):
            return pltpu.make_async_remote_copy(
                src_ref=src,
                dst_ref=target_slot(owner),
                send_sem=gt_send.at[index],
                recv_sem=gt_recv.at[index],
                device_id={"src": device},
                device_id_type=pl.DeviceIdType.MESH,
            )

        t_own = target_slot(s)
        t_out = [
            target_copy(target_ref, s, step, peer("src", step))
            for step in range(2, n_src, 2)
        ]
        for copy in t_out + s_out:
            copy.start()
        across = target_copy(target_ref, s, 1, partner)
        across.start()
        t_out.append(across)
        t_in = [target_copy(target_ref, partner, 1, partner)]
        own = [
            pltpu.make_async_copy(source_ref, s_own, own_sems.at[0]),
            pltpu.make_async_copy(target_ref, t_own, own_sems.at[1]),
        ]
    else:
        own = [
            pltpu.make_async_copy(source_ref, source_full, own_sems.at[0]),
            pltpu.make_async_copy(target_ref, target_full, own_sems.at[1]),
        ]
    for copy in own:
        copy.start()

    slots = plan_ref.shape[1]
    live = lax.broadcasted_iota(jnp.int32, (source_blocks, slots), 1) < count_ref[0, 0]
    near = lax.broadcasted_iota(jnp.int32, (source_blocks, slots), 0) == plan_ref[0:1, :]
    far = lax.broadcasted_iota(jnp.int32, (target_blocks, slots), 0) == plan_ref[1:2, :]
    near = jnp.where(near & live, 1.0, 0.0).astype(jnp.bfloat16)
    far = jnp.where(far, 1.0, 0.0).astype(jnp.bfloat16)
    kept = lax.dot_general(
        near, far, (((1,), (1,)), ((), ())), preferred_element_type=jnp.float32
    )
    for block in range(target_blocks):
        bias[block] = jnp.broadcast_to(
            jnp.where(kept[:, block : block + 1] > 0.5, 0.0, dead_score),
            (source_blocks, frames),
        )
    dual = start_ref[...] * log2_e
    sender = None
    potential[...] = dual

    diagonal = lax.broadcasted_iota(jnp.int32, (frames, frames), 0) == (
        lax.broadcasted_iota(jnp.int32, (frames, frames), 1)
    )

    for copy in own:
        copy.wait()
    if gather_here:
        for step in range(2, n_src, 2):
            owner = lax.rem(s + n_src - step, n_src)
            target_copy(target_ref, owner, step, owner).wait_recv()
            relay = target_copy(target_slot(owner), owner, step + 1, partner)
            relay.start()
            t_out.append(relay)
            owner = lax.rem(partner + n_src - step, n_src)
            t_in.append(target_copy(target_ref, owner, step + 1, partner))
        for copy in s_in + t_in:
            copy.wait_recv()

    def row_block(block, parts, make_scores):
        if make_scores:
            left = source_full[block].T
        peak = None
        for other in range(0, target_blocks, 2):
            if make_scores:
                right = jnp.concatenate(
                    [target_full[other], target_full[other + 1]], axis=1
                )
                product = jnp.dot(left, right, preferred_element_type=jnp.float32)
            for k in range(2):
                if make_scores:
                    tile = product[:, k * frames : (k + 1) * frames] * (
                        log2_e / smoothing_epsilon
                    ) + bias[other + k, pl.ds(block, 1), :]
                else:
                    tile = score[block, other + k]
                tile = tile + potential[other + k : other + k + 1, :]
                score[block, other + k] = tile
                peak = tile if peak is None else jnp.maximum(peak, tile)
        peak = jnp.max(peak, axis=1, keepdims=True)
        total = None
        for other in range(target_blocks):
            term = jnp.exp2(score[block, other] - peak)
            total = term if total is None else total + term
        total = jnp.sum(total, axis=1, keepdims=True)
        column = peak + jnp.log2(total)
        row = jnp.sum(jnp.where(diagonal, column, 0.0), axis=0, keepdims=True)
        parts[0, pl.ds(block, 1), :] = row

    def column_group_stats(first, parts):
        start = jnp.full((8, frames), 2 * dead_score, jnp.float32)

        def fold(value):
            return value.reshape(frames // 8, 8, frames)

        def peaks(block, current):
            raised = []
            for k in range(column_group):
                tile = score[block, first + k] + spread[block]
                score[block, first + k] = tile
                raised.append(jnp.maximum(current[k], jnp.max(fold(tile), axis=0)))
            return tuple(raised)

        peak = lax.fori_loop(0, source_blocks, peaks, (start,) * column_group, unroll=4)
        peak = [jnp.max(p, axis=0, keepdims=True) for p in peak]

        def sums(block, current):
            return tuple(
                current[k]
                + jnp.sum(fold(jnp.exp2(score[block, first + k] - peak[k])), axis=0)
                for k in range(column_group)
            )

        total = lax.fori_loop(
            0, source_blocks, sums, (jnp.zeros((8, frames), jnp.float32),) * column_group,
            unroll=4,
        )
        for k in range(column_group):
            parts[0, pl.ds(first + k, 1), :] = peak[k] + jnp.log2(
                jnp.sum(total[k], axis=0, keepdims=True)
            )

    sends = []

    def exchange(parts, send, recv, axis):
        copies = [
            remote(parts.at[0], parts.at[step], send.at[step], recv.at[step], axis, step)
            for step in range(1, sizes[axis])
        ]
        for copy in copies:
            copy.start()
        for copy in copies:
            copy.wait_recv()
        sends.extend(copies)
        return merge([parts[step] for step in range(sizes[axis])])

    for iteration in range(ITERS):
        parts = row_parts.at[iteration]

        def rows(block, carry):
            row_block(block, parts, iteration == 0)
            return carry

        lax.fori_loop(0, source_blocks, rows, 0, unroll=2)
        fresh = source_mass_ref[...] * log2_e - exchange(
            parts, row_send.at[iteration], row_recv.at[iteration], "tgt"
        )
        if sender is None:
            shift = sender = fresh
        else:
            shift, sender = fresh, fresh + sender
        if iteration == ITERS - 1:
            source_out[...] = sender * ln_2
        for block in range(source_blocks):
            column = jnp.sum(
                jnp.where(diagonal, shift[block : block + 1, :], 0.0),
                axis=1,
                keepdims=True,
            )
            spread[block] = jnp.broadcast_to(column, (frames, frames))
        parts = col_parts.at[iteration]

        def columns(group, carry):
            column_group_stats(group * column_group, parts)
            return carry

        lax.fori_loop(0, target_blocks // column_group, columns, 0)
        fresh = target_mass_ref[...] * log2_e - exchange(
            parts, col_send.at[iteration], col_recv.at[iteration], "src"
        )
        dual = fresh + dual
        if iteration == ITERS - 1:
            target_out[...] = dual * ln_2
        else:
            potential[...] = fresh

    if gather_here:
        sends.extend(s_out + t_out)
    for copy in sends:
        copy.wait_send()


def on_device(
    n_src,
    n_tgt,
    source_embed,
    target_embed,
    source_mass,
    target_mass,
    target_start,
    block_pairs,
    counts,
):
    source = jnp.swapaxes(source_embed, 1, 2)
    target = jnp.swapaxes(target_embed, 1, 2)
    source_blocks, source_width, frames = source.shape
    target_blocks, target_width, _ = target.shape
    gather_here = source_width % feature_tile == 0 and target_width % feature_tile == 0
    if not gather_here:
        source = lax.all_gather(source, "tgt", axis=1, tiled=True)
        target = lax.all_gather(target, "src", axis=1, tiled=True)
    features = source_width * n_tgt
    plan = block_pairs.reshape(block_pairs.shape[2], 2).T
    dma = pltpu.SemaphoreType.DMA
    vmem = pl.BlockSpec(memory_space=pltpu.VMEM)
    return pl.pallas_call(
        functools.partial(kernel, n_src, n_tgt, gather_here),
        out_shape=(
            jax.ShapeDtypeStruct(source_mass.shape, jnp.float32),
            jax.ShapeDtypeStruct(target_mass.shape, jnp.float32),
        ),
        in_specs=[vmem] * 6 + [pl.BlockSpec(memory_space=pltpu.SMEM)],
        out_specs=(vmem, vmem),
        scratch_shapes=[
            pltpu.VMEM((source_blocks, target_blocks, frames, frames), jnp.float32),
            pltpu.VMEM((source_blocks, features, frames), jnp.bfloat16),
            pltpu.VMEM((target_blocks, features, frames), jnp.bfloat16),
            pltpu.VMEM((source_blocks, frames, frames), jnp.float32),
            pltpu.VMEM((target_blocks, source_blocks, frames), jnp.float32),
            pltpu.VMEM((target_blocks, frames), jnp.float32),
            pltpu.VMEM((ITERS, n_tgt, source_blocks, frames), jnp.float32),
            pltpu.VMEM((ITERS, n_src, target_blocks, frames), jnp.float32),
            dma((2,)),
            dma((n_tgt,)),
            dma((n_tgt,)),
            dma((n_src,)),
            dma((n_src,)),
            dma((ITERS, n_tgt)),
            dma((ITERS, n_tgt)),
            dma((ITERS, n_src)),
            dma((ITERS, n_src)),
        ],
        compiler_params=pltpu.CompilerParams(
            collective_id=0, has_side_effects=True, vmem_limit_bytes=40 * 2**20
        ),
        name="sinkhorn",
    )(source, target, source_mass, target_mass, target_start, plan, counts)


def solution(mesh):
    in_specs = (
        P("src", None, "tgt"),
        P("tgt", None, "src"),
        P("src", None),
        P("tgt", None),
        P("tgt", None),
        P("src", "tgt", None, None),
        P("src", "tgt"),
    )
    out_specs = (P("src", None), P("tgt", None))
    return jax.shard_map(
        functools.partial(on_device, mesh.shape["src"], mesh.shape["tgt"]),
        mesh=mesh,
        in_specs=in_specs,
        out_specs=out_specs,
        check_vma=False,
    )
```
